256 devices in a mesh: ctx: 16 (over x_lo, z), tp: 8 (over y, x_hi), batch: 2 (over core).
Axes of the slice: x: 4 (x_hi: 2, x_lo: 2; x = x_hi * 2 + x_lo), y: 4, z: 8, core: 2. Of those that a mesh axis runs over, the one named last changes fastest.
Arguments:
- queries: bfloat16 [4, 2048, 128, 128], P('batch', 'ctx', 'tp'), may hold values from -60 to 60, as said below
- span_key_rows: bfloat16 [4, 2048, 8, 128], P('batch', 'ctx', 'tp'), may hold values from -6 to 6
- span_value_rows: bfloat16 [4, 2048, 8, 128], P('batch', 'ctx', 'tp'), may hold values from -1.5 to 1.5
- prefix_key_rows: bfloat16 [4, 4096, 8, 128], P('batch', 'ctx', 'tp'), may hold values from -6 to 6
- prefix_value_rows: bfloat16 [4, 4096, 8, 128], P('batch', 'ctx', 'tp'), may hold values from -1.5 to 1.5
- cached_len: int32 [4], P('batch'), may hold values from 1024 to 4096
- new_len: int32 [4], P('batch'), may hold values from 1024 to 2048
- prefill_flag: int32 [4], P('batch'), may hold values from 0 to 1, as said below
- block_order: int32 [32], replicated, may hold values from 0 to 31, each once
Outputs:
- attended: bfloat16 [4, 2048, 128, 128], P('batch', 'ctx', 'tp')
The draws below stay inside these ranges and needn't reach their ends.
Inputs may be any that keep to these rules, and one draw needn't show every extreme that they name: `queries`: large entries come in a few whole head vectors. `prefill_flag`: rows come in aligned pairs (rows 2k and 2k + 1): of each pair exactly one has the value 1.
All inputs are finite; a program needn't handle non-finite values.
Results may differ from the reference program's by a relative error of at most 0.012.
The reference program's roundings to bfloat16 on the way count: a program that leaves them out, or rounds other values in their place, can miss the bound.
Values may be sent and summed in bfloat16 or wider, within the bound.
A program may use at most 256 MiB of HBM per device.

```python
import jax
import jax.numpy as jnp
from jax import lax

QUERY_HEADS = 128
KEY_VALUE_HEADS = 8
HEAD_SIZE = 128
REQUEST_ROWS = 4
SPAN_SLOTS = 2048
CACHE_SLOTS = 4096
BLOCKS = 32
N_CTX = 16


def draw_queries(key, part):
    shape = (REQUEST_ROWS, SPAN_SLOTS, QUERY_HEADS, HEAD_SIZE)
    first = jax.random.fold_in(key, 0)
    values = jnp.clip(jax.random.normal(first, shape, jnp.float32), -6.0, 6.0)
    return values.astype(jnp.bfloat16)


def draw_prefill_flag(key, part):
    offsets = jax.random.randint(jax.random.fold_in(key, 7), (REQUEST_ROWS // 2,), 0, 2).astype(jnp.int32)
    paired = jnp.stack([offsets, 1 - offsets], 1)
    return paired.reshape(REQUEST_ROWS).astype(jnp.int32)


def plant(array, own_key, low, high):
    longest = array.shape.index(max(array.shape))
    spots = []
    for shift in (0, 1):
        where = [jax.random.randint(jax.random.fold_in(own_key, axis), (), 0, length) for axis, length in enumerate(array.shape)]
        where[longest] = (where[longest] + shift) % array.shape[longest]
        spots.append(tuple(where))
    return array.at[spots[0]].set(low).at[spots[1]].set(high)


def shard_levels(key, dims, pieces, smallest, largest):
    loudness, own = 1.0, jax.random.fold_in(key, 6)
    for position, shards_of in pieces:
        draws = jnp.exp(jax.random.uniform(jax.random.fold_in(own, position), (shards_of,), jnp.float32, smallest / len(pieces), largest / len(pieces)))
        loudness = loudness * jnp.repeat(draws, dims[position] // shards_of).reshape([-1 if axis == position else 1 for axis in range(len(dims))])
    return loudness


def centred(stream_key, extent, deviation, reach, pieces=(), kind=jnp.bfloat16):
    gain = shard_levels(stream_key, extent, pieces, -0.22, 0.18) if pieces else 1.0
    drawn = jax.random.normal(stream_key, extent, jnp.float32) * deviation * gain
    return jnp.minimum(jnp.maximum(drawn, -reach), reach).astype(kind)


def setup_inputs(seed: int = 0) -> dict:
    splits = jax.random.split(jax.random.key(seed), 10)
    return {
        "queries": draw_queries(jax.random.fold_in(splits[9], 71), 0),
        "span_key_rows": centred(splits[1], (REQUEST_ROWS, SPAN_SLOTS, KEY_VALUE_HEADS, HEAD_SIZE), 1.0, 6.0, ((0, 2), (1, 16), (2, 8))),
        "span_value_rows": centred(splits[2], (REQUEST_ROWS, SPAN_SLOTS, KEY_VALUE_HEADS, HEAD_SIZE), 0.25, 1.5, ((0, 2), (1, 16), (2, 8))),
        "prefix_key_rows": centred(splits[3], (REQUEST_ROWS, CACHE_SLOTS, KEY_VALUE_HEADS, HEAD_SIZE), 1.0, 6.0, ((0, 2), (1, 16), (2, 8))),
        "prefix_value_rows": centred(splits[4], (REQUEST_ROWS, CACHE_SLOTS, KEY_VALUE_HEADS, HEAD_SIZE), 0.25, 1.5, ((0, 2), (1, 16), (2, 8))),
        "cached_len": plant(jax.random.randint(splits[5], (REQUEST_ROWS,), CACHE_SLOTS // 4, CACHE_SLOTS + 1), jax.random.fold_in(splits[5], 1), CACHE_SLOTS // 4, CACHE_SLOTS).astype(jnp.int32),
        "new_len": plant(jax.random.randint(splits[6], (REQUEST_ROWS,), SPAN_SLOTS // 2, SPAN_SLOTS + 1), jax.random.fold_in(splits[6], 1), SPAN_SLOTS // 2, SPAN_SLOTS).astype(jnp.int32),
        "prefill_flag": draw_prefill_flag(jax.random.fold_in(splits[9], 71), 0),
        "block_order": jax.random.permutation(splits[8], BLOCKS).astype(jnp.int32),
    }


rope_base = 500000.0
neg_large = -1.0e30


def rotate(x, positions):
    half = x.shape[-1] // 2
    inverse = rope_base ** (-(jnp.arange(half, dtype=jnp.float32) * 2.0 / x.shape[-1]))
    angle = positions.astype(jnp.float32)[:, :, None, None] * inverse
    cosine = jnp.cos(angle)
    sine = jnp.sin(angle)
    wide = x.astype(jnp.float32)
    first = wide[..., :half]
    second = wide[..., half:]
    return jnp.concatenate([first * cosine - second * sine, second * cosine + first * sine], -1).astype(jnp.bfloat16)


def reference(queries, span_key_rows, span_value_rows, prefix_key_rows, prefix_value_rows, cached_len, new_len, prefill_flag, block_order):
    nblocks = 2 * N_CTX
    blk = SPAN_SLOTS // nblocks
    query_group = QUERY_HEADS // KEY_VALUE_HEADS
    qblock = min(512, SPAN_SLOTS)
    nqb = SPAN_SLOTS // qblock
    scale = 1.0 / (HEAD_SIZE ** 0.5)

    def to_logical(x):
        split = x.reshape((REQUEST_ROWS, nblocks, blk) + x.shape[2:])
        return jnp.zeros_like(split).at[:, block_order].set(split).reshape(x.shape)

    logical_q = to_logical(queries)
    logical_k = to_logical(span_key_rows)
    logical_v = to_logical(span_value_rows)
    index = jnp.arange(SPAN_SLOTS, dtype=jnp.int32)
    base = jnp.where(prefill_flag == 1, 0, cached_len).astype(jnp.int32)
    positions = base[:, None] + index[None, :]
    q_rot = rotate(logical_q, positions)
    k_rot = rotate(logical_k, positions)
    keys = jnp.concatenate([prefix_key_rows, k_rot], 1)
    values = jnp.concatenate([prefix_value_rows, logical_v], 1)
    cache_index = jnp.arange(CACHE_SLOTS, dtype=jnp.int32)

    def one_row(items):
        query_row, k_row, v_row, clen, nlen, flag = items
        query_heads = jnp.moveaxis(query_row.reshape(SPAN_SLOTS, KEY_VALUE_HEADS, query_group, HEAD_SIZE), 1, 0)
        heads_k = jnp.moveaxis(k_row, 1, 0)
        heads_v = jnp.moveaxis(v_row, 1, 0)
        cache_ok = (cache_index < clen) & (flag == 0)

        def one_head(hitems):
            qh, kh, vh = hitems
            kf = kh.astype(jnp.float32)
            vf = vh.astype(jnp.float32)
            blocks = qh.reshape(nqb, qblock, query_group, HEAD_SIZE)

            def one_block(bitems):
                qb, start = bitems
                qi = start + jnp.arange(qblock, dtype=jnp.int32)
                new_ok = (index[None, :] <= qi[:, None]) & (index[None, :] < nlen)
                valid = jnp.concatenate([jnp.broadcast_to(cache_ok[None, :], (qblock, CACHE_SLOTS)), new_ok], 1)
                score = jnp.einsum("qgd,nd->gqn", qb.astype(jnp.float32), kf) * scale
                score = jnp.where(valid[None], score, neg_large)
                top = jnp.max(score, -1, keepdims=True)
                prob = jnp.where(valid[None], jnp.exp(score - top), 0.0)
                total = jnp.sum(prob, -1)
                rounded = lax.optimization_barrier(prob.astype(jnp.bfloat16)).astype(jnp.float32)
                summed = jnp.einsum("gqn,nd->qgd", rounded, vf)
                out = summed / jnp.moveaxis(total, 0, 1)[:, :, None]
                return jnp.where((qi < nlen)[:, None, None], out, 0.0)

            starts = jnp.arange(nqb, dtype=jnp.int32) * qblock
            return lax.map(one_block, (blocks, starts)).reshape(SPAN_SLOTS, query_group, HEAD_SIZE)

        per_head = lax.map(one_head, (query_heads, heads_k, heads_v))
        return jnp.moveaxis(per_head, 0, 1).reshape(SPAN_SLOTS, QUERY_HEADS, HEAD_SIZE)

    logical_out = lax.map(one_row, (q_rot, keys, values, cached_len, new_len, prefill_flag))
    stored = logical_out.reshape(REQUEST_ROWS, nblocks, blk, QUERY_HEADS, HEAD_SIZE)[:, block_order]
    return stored.reshape(REQUEST_ROWS, SPAN_SLOTS, QUERY_HEADS, HEAD_SIZE).astype(jnp.bfloat16)
```

```python
import functools
import math

import jax
import jax.numpy as jnp
from jax import lax
from jax.experimental import pallas as pl
from jax.experimental.pallas import tpu as pltpu
from jax.sharding import PartitionSpec as P

ROPE_BASE = 500000.0
NEG = -1e30
TILE = 256
MESH = pl.DeviceIdType.MESH


def trig_tables(positions, size):
    half = size // 2
    inverse = ROPE_BASE ** (-(jnp.arange(half, dtype=jnp.float32) * 2.0 / size))
    angle = positions.astype(jnp.float32)[:, :, None] * inverse
    cosine, sine = jnp.cos(angle), jnp.sin(angle)
    return jnp.concatenate([cosine, cosine], -1), jnp.concatenate([-sine, sine], -1)


def prep_kernel(flag, cos, sin, sk, sv, ck, cv, f_out, g_out):
    half = sk.shape[-1] // 2
    a = flag[0]
    for piece, row in enumerate((a, 1 - a)):
        x = sk[row].astype(jnp.float32)
        turned = x * cos[row] + pltpu.roll(x, half, 1) * sin[row]
        f_out[piece] = turned.astype(jnp.bfloat16)
        f_out[2 + piece] = sv[row].astype(jnp.float32).T.astype(jnp.bfloat16)
    n = ck.shape[1] // 2
    for part in range(2):
        g_out[part] = ck[a, part * n : (part + 1) * n]
        g_out[2 + part] = cv[a, part * n : (part + 1) * n].astype(jnp.float32).T.astype(jnp.bfloat16)


def main_kernel(
    nz, flag, clen, nlen, order, q, cos, sin, fown, gown, out,
    fbuf, gbuf, qt, kx, vx, s0, s1, acc, top, tot,
    f_send, f_recv, g_send, g_recv, gz_send, gz_recv,
):
    me = lax.axis_index("ctx")
    column, z = me // nz, me % nz
    other = (1 - column) * nz + z

    def mine(d):
        return column * nz + (z + d + nz) % nz

    def theirs(d):
        return (1 - column) * nz + (z + d + nz) % nz

    up, down = mine(1), mine(-1)

    barrier = pltpu.get_barrier_semaphore()
    for peer in (up, down, other):
        pl.semaphore_signal(barrier, inc=1, device_id={"ctx": peer}, device_id_type=MESH)
    pl.semaphore_wait(barrier, 3)

    started = []
    counts = {"f": 0, "g": 0, "z": 0}
    sends = {"f": f_send, "g": g_send, "z": gz_send}
    recvs = {"f": f_recv, "g": g_recv, "z": gz_recv}

    def send(kind, src, dst, slot, peer):
        c = pltpu.make_async_remote_copy(
            src_ref=src, dst_ref=dst, send_sem=sends[kind].at[counts[kind]], recv_sem=recvs[kind].at[slot],
            device_id={"ctx": peer}, device_id_type=MESH,
        )
        counts[kind] += 1
        c.start()
        started.append(c)

    def send_f(slot, peer, own=False):
        send("f", fown if own else fbuf.at[slot], fbuf.at[slot], slot, peer)

    def send_g(slot, peer, own=False):
        send("g", gown if own else gbuf.at[slot], gbuf.at[slot], slot, peer)

    def send_half(slot, part, peer):
        ref = gbuf.at[slot, pl.ds(2 * part, 2)]
        send("z", ref, ref, part, peer)

    def got(buf, sem):
        pltpu.make_async_remote_copy(
            src_ref=buf, dst_ref=buf, send_sem=f_send.at[0], recv_sem=sem, device_id={"ctx": other}, device_id_type=MESH
        ).wait_recv()

    def got_f(slot):
        got(fbuf.at[slot], f_recv.at[slot])

    def got_g(slot):
        got(gbuf.at[slot], g_recv.at[slot])

    send_g(me, up, True)
    send_g(me, down, True)
    send_f(me, other, True)
    send_f(me, up, True)
    send_f(me, down, True)
    send_g(me, other, True)

    rows, count, heads, size = q.shape
    half = size // 2
    group = TILE // heads
    tiles = count // group
    swap = flag[0] == 1
    scale = math.log2(math.e) / math.sqrt(size)

    def prepare(t, _):
        here = pl.ds(pl.multiple_of(t * group, group), group)
        turned = []
        for r in range(rows):
            x = q[r, here].astype(jnp.float32)
            c, s = cos[r, here], sin[r, here]
            y = x * c[:, None, :] + pltpu.roll(x, half, 2) * s[:, None, :]
            turned.append(y.reshape(TILE, size))
        place = t * group + lax.broadcasted_iota(jnp.int32, (size, TILE), 1) // heads
        hot = jnp.where(lax.broadcasted_iota(jnp.int32, (size, TILE), 0) == place, 1.0, 0.0).astype(jnp.bfloat16)
        for r, y in enumerate((jnp.where(swap, turned[1], turned[0]), jnp.where(swap, turned[0], turned[1]))):
            at = r * tiles + t
            qt[at, 0:size] = y.T.astype(jnp.bfloat16)
            qt[at, size : 2 * size] = hot
            acc[at] = jnp.zeros((size, TILE), jnp.float32)
            top[at] = jnp.full((1, TILE), NEG, jnp.float32)
            tot[at] = jnp.zeros((1, TILE), jnp.float32)
        return 0

    lax.fori_loop(0, tiles, prepare, 0)

    piece = fown.shape[1]
    cached = jnp.where(swap, clen[1], clen[0])
    live = (jnp.where(swap, nlen[1], nlen[0]), jnp.where(swap, nlen[0], nlen[1]))
    blk = piece // 2
    lane = lax.broadcasted_iota(jnp.int32, (piece, size), 1)
    line = lax.broadcasted_iota(jnp.int32, (piece, size), 0)

    def logical(slot, i):
        first, second = order[2 * slot], order[2 * slot + 1]
        return jnp.where(i < blk, first * blk + i, second * blk + i - blk)

    q_index = logical(me, lane)

    def bias(visible):
        return jnp.where(visible, 0.0, NEG).astype(jnp.bfloat16)

    def scores(at, row):
        return jnp.dot(kx[row], qt[at], preferred_element_type=jnp.float32)

    def absorb(s_ref, at, row):
        s = s_ref[...]
        old = top[at]
        new = jnp.maximum(old, jnp.max(s, axis=0, keepdims=True))
        p = jnp.exp2((s - new) * scale)
        fade = jnp.exp2((old - new) * scale)
        tot[at] = tot[at] * fade + jnp.sum(p, axis=0, keepdims=True)
        acc[at] = acc[at] * fade + jnp.dot(vx[row], p.astype(jnp.bfloat16), preferred_element_type=jnp.float32)
        top[at] = new

    def compute(total):
        s0[...] = scores(0, 0)

        def step(u, _):
            t0 = 2 * u
            t1, t2 = t0 + 1, jnp.minimum(t0 + 2, total - 1)
            s1[...] = scores(t1, t1 // tiles)
            absorb(s0, t0, t0 // tiles)
            s0[...] = scores(t2, t2 // tiles)
            absorb(s1, t1, t1 // tiles)
            return 0

        lax.fori_loop(0, total // 2, step, 0)

    def cache_chunk(*blocks):
        for j, (ref, slot) in enumerate(blocks):
            for h in range(2):
                at = (2 * j + h) * piece
                kx[0, at : at + piece, 0:size] = ref[h]
                kx[0, at : at + piece, size : 2 * size] = bias(slot * 2 * piece + h * piece + line < cached)
                vx[0, :, at : at + piece] = ref[2 + h]
        compute(tiles)

    def span_chunk(*blocks):
        for j, (ref, slot) in enumerate(blocks):
            at = j * piece
            k_index = logical(slot, line)
            for r in range(2):
                kx[r, at : at + piece, 0:size] = ref[r]
                kx[r, at : at + piece, size : 2 * size] = bias((k_index <= q_index) & (k_index < live[r]))
                vx[r, :, at : at + piece] = ref[2 + r]
        compute(2 * tiles)

    def gb(slot):
        return gbuf.at[slot], slot

    def fb(slot):
        return fbuf.at[slot], slot

    last = nz // 2

    got_f(other)
    send_f(other, up)
    send_f(other, down)
    for d in (1, -1):
        got_g(mine(d))
        send_g(mine(d), down if d > 0 else up)
        send_g(mine(d), other)
    cache_chunk(gb(mine(1)), gb(mine(-1)))
    for d in (1, -1):
        got_f(mine(d))
        send_f(mine(d), down if d > 0 else up)
    got_g(other)
    cache_chunk((gown, me), gb(other))
    for d in (1, -1):
        got_f(theirs(d))
        send_f(theirs(d), down if d > 0 else up)
    for d in (2, -2):
        got_g(mine(d))
        send_g(mine(d), down if d > 0 else up)
        send_g(mine(d), other)
    span_chunk((fown, me), fb(other), fb(mine(1)), fb(mine(-1)))
    for d in (2, -2):
        got_f(mine(d))
        send_f(mine(d), down if d > 0 else up)
    got_g(theirs(1))
    got_g(theirs(-1))
    cache_chunk(gb(theirs(1)), gb(theirs(-1)))
    for d in (2, -2):
        got_f(theirs(d))
        send_f(theirs(d), down if d > 0 else up)
    for d in (3, -3):
        got_g(mine(d))
        send_half(mine(d), 0 if d < 0 else 1, up if d < 0 else down)
        send_g(mine(d), other)
    cache_chunk(gb(mine(2)), gb(mine(-2)))
    far = mine(last)
    for part in range(2):
        got(gbuf.at[far, pl.ds(2 * part, 2)], gz_recv.at[part])
    send_g(far, other)
    span_chunk(fb(theirs(1)), fb(theirs(-1)), fb(mine(2)), fb(mine(-2)))
    got_f(mine(3))
    got_f(mine(-3))
    send_f(mine(-3), up)
    got_g(theirs(2))
    got_g(theirs(-2))
    cache_chunk(gb(theirs(2)), gb(theirs(-2)))
    got_f(theirs(3))
    got_f(theirs(-3))
    send_f(theirs(3), down)
    cache_chunk(gb(mine(3)), gb(mine(-3)))
    span_chunk(fb(theirs(2)), fb(theirs(-2)), fb(mine(3)), fb(mine(-3)))
    got_g(theirs(3))
    got_g(theirs(-3))
    cache_chunk(gb(theirs(3)), gb(theirs(-3)))
    got_g(theirs(last))
    cache_chunk(gb(far), gb(theirs(last)))
    got_f(far)
    got_f(theirs(last))
    span_chunk(fb(theirs(3)), fb(theirs(-3)), fb(far), fb(theirs(last)))

    def finish(t, _):
        here = pl.ds(pl.multiple_of(t * group, group), group)
        done = [(acc[r * tiles + t] / tot[r * tiles + t]).T.reshape(group, heads, size) for r in range(2)]
        i = logical(me, t * group + lax.broadcasted_iota(jnp.int32, (group, heads, size), 0))
        for r in range(2):
            value = jnp.where(swap, done[1 - r], done[r])
            out[r, here] = jnp.where(i < nlen[r], value, 0.0).astype(out.dtype)
        return 0

    lax.fori_loop(0, tiles, finish, 0)
    for c in started:
        c.wait_send()


def shards(nz, queries, span_k, span_v, cache_k, cache_v, cached_len, new_len, prefill_flag, block_order):
    rows, count, heads, size = queries.shape
    n_ctx = lax.axis_size("ctx")
    nblocks = block_order.shape[0]
    blk = count * n_ctx // nblocks
    me = lax.axis_index("ctx")
    index = (lax.dynamic_slice(block_order, (2 * me,), (2,))[:, None] * blk + jnp.arange(blk, dtype=jnp.int32)).reshape(count)
    base = jnp.where(prefill_flag == 1, 0, cached_len)
    cos, sin = trig_tables(base[:, None] + index[None, :], size)

    smem = pl.BlockSpec(memory_space=pltpu.SMEM)
    vmem = pl.BlockSpec(memory_space=pltpu.VMEM)
    packed = jax.ShapeDtypeStruct((4, count, size), jnp.bfloat16)
    fown, gown = pl.pallas_call(
        prep_kernel,
        out_shape=(packed, packed),
        in_specs=[smem] + [vmem] * 6,
        out_specs=(vmem, vmem),
        name="prep",
    )(prefill_flag, cos, sin, span_k[:, :, 0], span_v[:, :, 0], cache_k[:, :, 0], cache_v[:, :, 0])

    tiles = count * heads // TILE
    keys = 4 * count
    bf16, f32, dma = jnp.bfloat16, jnp.float32, pltpu.SemaphoreType.DMA
    return pl.pallas_call(
        functools.partial(main_kernel, nz),
        out_shape=jax.ShapeDtypeStruct(queries.shape, queries.dtype),
        in_specs=[smem] * 4 + [vmem] * 5,
        out_specs=vmem,
        scratch_shapes=[
            pltpu.VMEM((n_ctx, 4, count, size), bf16),
            pltpu.VMEM((n_ctx, 4, count, size), bf16),
            pltpu.VMEM((2 * tiles, 2 * size, TILE), bf16),
            pltpu.VMEM((2, keys, 2 * size), bf16),
            pltpu.VMEM((2, size, keys), bf16),
            pltpu.VMEM((keys, TILE), f32),
            pltpu.VMEM((keys, TILE), f32),
            pltpu.VMEM((2 * tiles, size, TILE), f32),
            pltpu.VMEM((2 * tiles, 1, TILE), f32),
            pltpu.VMEM((2 * tiles, 1, TILE), f32),
            dma((2 * n_ctx,)),
            dma((n_ctx,)),
            dma((2 * n_ctx,)),
            dma((n_ctx,)),
            dma((2,)),
            dma((2,)),
        ],
        compiler_params=pltpu.CompilerParams(collective_id=0, has_side_effects=True, vmem_limit_bytes=48 * 1024 * 1024),
        name="gather_attend",
    )(prefill_flag, cached_len, new_len, block_order, queries, cos, sin, fown, gown)


def solution(mesh):
    nz = mesh.shape["ctx"] // 2
    four = P("batch", "ctx", "tp", None)
    return jax.shard_map(
        functools.partial(shards, nz),
        mesh=mesh,
        in_specs=(four,) * 5 + (P("batch"),) * 3 + (P(),),
        out_specs=four,
        check_vma=False,
    )
```

```python
import functools
import math

import jax
import jax.numpy as jnp
from jax import lax
from jax.experimental import pallas as pl
from jax.experimental.pallas import tpu as pltpu
from jax.sharding import PartitionSpec as P

ROPE_BASE = 500000.0
NEG = -1e30
TILE = 256
MESH = pl.DeviceIdType.MESH


HALF_PI = (1.5703125, 4.837512969970703125e-4, 7.54978995489188216e-8)


def turn_tables(positions, inverse, sign):
    angle = positions * inverse
    quarter = jnp.floor(angle * (2.0 / math.pi) + 0.5)
    x = ((angle - quarter * HALF_PI[0]) - quarter * HALF_PI[1]) - quarter * HALF_PI[2]
    z = x * x
    sine = ((-1.9515295891e-4 * z + 8.3321608736e-3) * z - 1.6666654611e-1) * z * x + x
    cosine = ((2.443315711809948e-5 * z - 1.388731625493765e-3) * z + 4.166664568298827e-2) * z * z - 0.5 * z + 1.0
    n = quarter.astype(jnp.int32)
    odd = (n & 1) == 1
    c = jnp.where(odd, sine, cosine)
    s = jnp.where(odd, cosine, sine)
    c = jnp.where(((n + 1) & 2) == 2, -c, c)
    s = jnp.where((n & 2) == 2, -s, s)
    return c, s * sign


def main_kernel(
    nz, flag, clen, nlen, order, q_hbm, sk_hbm, sv_hbm, ck_hbm, cv_hbm, out,
    q, sk, sv, ck, cv, cos, sin, fbuf, gbuf, qt, kx, vx, s_tiles, m_tiles, acc, top, tot,
    in_sem, f_send, f_recv, g_send, g_recv, gz_send, gz_recv,
):
    loads = [
        pltpu.make_async_copy(src, dst, in_sem.at[i])
        for i, (src, dst) in enumerate(((ck_hbm, ck), (cv_hbm, cv), (sk_hbm, sk), (sv_hbm, sv), (q_hbm, q)))
    ]
    for c in loads:
        c.start()
    me = lax.axis_index("ctx")
    column, z = me // nz, me % nz
    other = (1 - column) * nz + z

    def mine(d):
        return column * nz + (z + d + nz) % nz

    def theirs(d):
        return (1 - column) * nz + (z + d + nz) % nz

    up, down = mine(1), mine(-1)

    barrier = pltpu.get_barrier_semaphore()
    for peer in (up, down, other):
        pl.semaphore_signal(barrier, inc=1, device_id={"ctx": peer}, device_id_type=MESH)

    rows, count, heads, size = q.shape
    half = size // 2
    group = TILE // heads
    tiles = count // group
    piece = fbuf.shape[2]
    blk = piece // 2
    swap = flag[0] == 1
    scale = math.log2(math.e) / math.sqrt(size)
    cached = jnp.where(swap, clen[1], clen[0])
    live = (jnp.where(swap, nlen[1], nlen[0]), jnp.where(swap, nlen[0], nlen[1]))
    lane = lax.broadcasted_iota(jnp.int32, (piece, size), 1)
    line = lax.broadcasted_iota(jnp.int32, (piece, size), 0)

    def logical(slot, i):
        first, second = order[2 * slot], order[2 * slot + 1]
        return jnp.where(i < blk, first * blk + i, second * blk + i - blk)

    def pick(ref, r, at=slice(None)):
        return jnp.where(swap, ref[1 - r, at].astype(jnp.float32), ref[r, at].astype(jnp.float32))

    loads[0].wait()
    loads[1].wait()
    for h in range(2):
        at = slice(h * piece, (h + 1) * piece)
        gbuf[me, h] = pick(ck, 0, at).astype(jnp.bfloat16)
        gbuf[me, 2 + h] = pick(cv, 0, at).T.astype(jnp.bfloat16)
    loads[2].wait()
    loads[3].wait()
    k = (lane % half).astype(jnp.float32)
    inverse = jnp.exp2(k * (-2.0 / size * math.log2(ROPE_BASE)))
    sign = jnp.where(lane < half, -1.0, 1.0)
    index = logical(me, line)
    for r, base in enumerate((cached, 0)):
        cos[r], sin[r] = turn_tables((index + base).astype(jnp.float32), inverse, sign)
        x = pick(sk, r)
        fbuf[me, r] = (x * cos[r] + pltpu.roll(x, half, 1) * sin[r]).astype(jnp.bfloat16)
        fbuf[me, 2 + r] = pick(sv, r).T.astype(jnp.bfloat16)

    pl.semaphore_wait(barrier, 3)
    started = []
    counts = {"f": 0, "g": 0, "z": 0}
    sends = {"f": f_send, "g": g_send, "z": gz_send}
    recvs = {"f": f_recv, "g": g_recv, "z": gz_recv}

    def send(kind, src, dst, slot, peer):
        c = pltpu.make_async_remote_copy(
            src_ref=src, dst_ref=dst, send_sem=sends[kind].at[counts[kind]], recv_sem=recvs[kind].at[slot],
            device_id={"ctx": peer}, device_id_type=MESH,
        )
        counts[kind] += 1
        c.start()
        started.append(c)

    def send_f(slot, peer):
        send("f", fbuf.at[slot], fbuf.at[slot], slot, peer)

    def send_g(slot, peer):
        send("g", gbuf.at[slot], gbuf.at[slot], slot, peer)

    def send_half(slot, part, peer):
        ref = gbuf.at[slot, pl.ds(2 * part, 2)]
        send("z", ref, ref, part, peer)

    def got(buf, sem):
        pltpu.make_async_remote_copy(
            src_ref=buf, dst_ref=buf, send_sem=f_send.at[0], recv_sem=sem, device_id={"ctx": other}, device_id_type=MESH
        ).wait_recv()

    def got_f(slot):
        got(fbuf.at[slot], f_recv.at[slot])

    def got_g(slot):
        got(gbuf.at[slot], g_recv.at[slot])

    send_g(me, up)
    send_g(me, down)
    send_f(me, other)
    send_f(me, up)
    send_f(me, down)
    send_g(me, other)

    loads[4].wait()

    def prepare(t, _):
        here = pl.ds(pl.multiple_of(t * group, group), group)
        place = t * group + lax.broadcasted_iota(jnp.int32, (size, TILE), 1) // heads
        hot = jnp.where(lax.broadcasted_iota(jnp.int32, (size, TILE), 0) == place, 1.0, 0.0).astype(jnp.bfloat16)
        for r in range(rows):
            at = r * tiles + t
            x = pick(q, r, here)
            y = x * cos[r, here][:, None, :] + pltpu.roll(x, half, 2) * sin[r, here][:, None, :]
            qt[at, 0:size] = y.reshape(TILE, size).T.astype(jnp.bfloat16)
            qt[at, size : 2 * size] = hot
            acc[at] = jnp.zeros((size, TILE), jnp.float32)
            top[at] = jnp.full((1, TILE), NEG, jnp.float32)
            tot[at] = jnp.zeros((1, TILE), jnp.float32)
        return 0

    lax.fori_loop(0, tiles, prepare, 0)

    q_index = logical(me, lane)

    def bias(visible):
        return jnp.where(visible, 0.0, NEG).astype(jnp.bfloat16)

    def scores(t, at, row):
        s = jnp.dot(kx[row], qt[at], preferred_element_type=jnp.float32)
        s_tiles[t][...] = s
        m_tiles[t][...] = jnp.max(s, axis=0, keepdims=True)

    def absorb(t, at, row):
        old = top[at]
        new = jnp.maximum(old, m_tiles[t][...])
        p = jnp.exp2((s_tiles[t][...] - new) * scale)
        fade = jnp.exp2((old - new) * scale)
        tot[at] = tot[at] * fade + jnp.sum(p, axis=0, keepdims=True)
        acc[at] = acc[at] * fade + jnp.dot(vx[row], p.astype(jnp.bfloat16), preferred_element_type=jnp.float32)
        top[at] = new

    def compute(row):
        ahead = 2
        for t in range(ahead):
            scores(t, row * tiles + t, row)
        for t in range(tiles):
            if t + ahead < tiles:
                scores(t + ahead, row * tiles + t + ahead, row)
            absorb(t, row * tiles + t, row)

    def cache_chunk(*blocks):
        for j, (ref, slot) in enumerate(blocks):
            for h in range(2):
                at = (2 * j + h) * piece
                kx[0, at : at + piece, 0:size] = ref[h]
                kx[0, at : at + piece, size : 2 * size] = bias(slot * 2 * piece + h * piece + line < cached)
                vx[0, :, at : at + piece] = ref[2 + h]
        compute(0)

    def span_chunk(*blocks):
        for j, (ref, slot) in enumerate(blocks):
            at = j * piece
            k_index = logical(slot, line)
            for r in range(2):
                kx[r, at : at + piece, 0:size] = ref[r]
                kx[r, at : at + piece, size : 2 * size] = bias((k_index <= q_index) & (k_index < live[r]))
                vx[r, :, at : at + piece] = ref[2 + r]

        def one(r, _):
            compute(r)
            return 0

        lax.fori_loop(0, 2, one, 0)

    def gb(slot):
        return gbuf.at[slot], slot

    def fb(slot):
        return fbuf.at[slot], slot

    last = nz // 2

    def on(d):
        return down if d > 0 else up

    def pass_f(*slots):
        for slot, d in slots:
            got_f(slot)
            send_f(slot, on(d))

    def pass_g(*distances):
        for d in distances:
            got_g(mine(d))
            send_g(mine(d), on(d))
            send_g(mine(d), other)

    got_f(other)
    send_f(other, up)
    send_f(other, down)
    pass_g(1, -1)
    cache_chunk(gb(mine(1)), gb(mine(-1)))
    pass_f((mine(1), 1), (mine(-1), -1))
    got_g(other)
    cache_chunk(gb(me), gb(other))
    span_chunk(fb(me), fb(other), fb(mine(1)), fb(mine(-1)))
    pass_f((theirs(1), 1), (theirs(-1), -1))
    pass_g(2, -2)
    got_g(theirs(1))
    got_g(theirs(-1))
    cache_chunk(gb(theirs(1)), gb(theirs(-1)))
    cache_chunk(gb(mine(2)), gb(mine(-2)))
    pass_f((mine(2), 2), (mine(-2), -2))
    span_chunk(fb(theirs(1)), fb(theirs(-1)), fb(mine(2)), fb(mine(-2)))
    pass_f((theirs(2), 2), (theirs(-2), -2))
    for d in (3, -3):
        got_g(mine(d))
        send_half(mine(d), 0 if d < 0 else 1, on(d))
        send_g(mine(d), other)
    got_g(theirs(2))
    got_g(theirs(-2))
    cache_chunk(gb(theirs(2)), gb(theirs(-2)))
    cache_chunk(gb(mine(3)), gb(mine(-3)))
    got_f(mine(3))
    got_f(mine(-3))
    send_f(mine(-3), up)
    span_chunk(fb(theirs(2)), fb(theirs(-2)), fb(mine(3)), fb(mine(-3)))
    got_f(theirs(3))
    got_f(theirs(-3))
    send_f(theirs(3), down)
    far = mine(nz // 2)
    for part in range(2):
        got(gbuf.at[far, pl.ds(2 * part, 2)], gz_recv.at[part])
    send_g(far, other)
    got_g(theirs(3))
    got_g(theirs(-3))
    cache_chunk(gb(theirs(3)), gb(theirs(-3)))
    got_f(far)
    got_f(theirs(nz // 2))
    span_chunk(fb(theirs(3)), fb(theirs(-3)), fb(far), fb(theirs(nz // 2)))
    got_g(theirs(nz // 2))
    cache_chunk(gb(far), gb(theirs(nz // 2)))

    def finish(t, _):
        here = pl.ds(pl.multiple_of(t * group, group), group)
        done = [(acc[r * tiles + t] / tot[r * tiles + t]).T.reshape(group, heads, size) for r in range(2)]
        i = logical(me, t * group + lax.broadcasted_iota(jnp.int32, (group, heads, size), 0))
        for r in range(2):
            value = jnp.where(swap, done[1 - r], done[r])
            out[r, here] = jnp.where(i < nlen[r], value, 0.0).astype(out.dtype)
        return 0

    lax.fori_loop(0, tiles, finish, 0)
    for c in started:
        c.wait_send()


def shards(nz, queries, span_k, span_v, cache_k, cache_v, cached_len, new_len, prefill_flag, block_order):
    rows, count, heads, size = queries.shape
    n_ctx = lax.axis_size("ctx")
    smem = pl.BlockSpec(memory_space=pltpu.SMEM)
    hbm = pl.BlockSpec(memory_space=pl.ANY)
    vmem = pl.BlockSpec(memory_space=pltpu.VMEM)
    tiles = count * heads // TILE
    keys = 4 * count
    bf16, f32, dma = jnp.bfloat16, jnp.float32, pltpu.SemaphoreType.DMA
    inputs = [queries] + [a[:, :, 0] for a in (span_k, span_v, cache_k, cache_v)]
    return pl.pallas_call(
        functools.partial(main_kernel, nz),
        out_shape=jax.ShapeDtypeStruct(queries.shape, queries.dtype),
        in_specs=[smem] * 4 + [hbm] * 5,
        out_specs=vmem,
        scratch_shapes=[pltpu.VMEM(a.shape, bf16) for a in inputs]
        + [
            pltpu.VMEM((rows, count, size), f32),
            pltpu.VMEM((rows, count, size), f32),
            pltpu.VMEM((n_ctx, 4, count, size), bf16),
            pltpu.VMEM((n_ctx, 4, count, size), bf16),
            pltpu.VMEM((2 * tiles, 2 * size, TILE), bf16),
            pltpu.VMEM((2, keys, 2 * size), bf16),
            pltpu.VMEM((2, size, keys), bf16),
            [pltpu.VMEM((keys, TILE), f32)] * tiles,
            [pltpu.VMEM((1, TILE), f32)] * tiles,
            pltpu.VMEM((2 * tiles, size, TILE), f32),
            pltpu.VMEM((2 * tiles, 1, TILE), f32),
            pltpu.VMEM((2 * tiles, 1, TILE), f32),
            dma((5,)),
            dma((2 * n_ctx,)),
            dma((n_ctx,)),
            dma((2 * n_ctx,)),
            dma((n_ctx,)),
            dma((2,)),
            dma((2,)),
        ],
        compiler_params=pltpu.CompilerParams(collective_id=0, has_side_effects=True, vmem_limit_bytes=67043328),
        name="gather_attend",
    )(prefill_flag, cached_len, new_len, block_order, *inputs)


def solution(mesh):
    nz = mesh.shape["ctx"] // 2
    four = P("batch", "ctx", "tp", None)
    return jax.shard_map(
        functools.partial(shards, nz),
        mesh=mesh,
        in_specs=(four,) * 5 + (P("batch"),) * 3 + (P(),),
        out_specs=four,
        check_vma=False,
    )
```

```python
import functools
import math

import jax
import jax.numpy as jnp
from jax import lax
from jax.experimental import pallas as pl
from jax.experimental.pallas import tpu as pltpu
from jax.sharding import PartitionSpec as P

ROPE_BASE = 500000.0
NEG = -1e30
TILE = 256
MESH = pl.DeviceIdType.MESH


HALF_PI = (1.5703125, 4.837512969970703125e-4, 7.54978995489188216e-8)


def turn_tables(positions, inverse, sign):
    angle = positions * inverse
    quarter = jnp.floor(angle * (2.0 / math.pi) + 0.5)
    x = ((angle - quarter * HALF_PI[0]) - quarter * HALF_PI[1]) - quarter * HALF_PI[2]
    z = x * x
    sine = ((-1.9515295891e-4 * z + 8.3321608736e-3) * z - 1.6666654611e-1) * z * x + x
    cosine = ((2.443315711809948e-5 * z - 1.388731625493765e-3) * z + 4.166664568298827e-2) * z * z - 0.5 * z + 1.0
    n = quarter.astype(jnp.int32)
    odd = (n & 1) == 1
    c = jnp.where(odd, sine, cosine)
    s = jnp.where(odd, cosine, sine)
    c = jnp.where(((n + 1) & 2) == 2, -c, c)
    s = jnp.where((n & 2) == 2, -s, s)
    return c, s * sign


def main_kernel(
    nz, flag, clen, nlen, order, q_hbm, sk_hbm, sv_hbm, ck_hbm, cv_hbm, out,
    q, sk, sv, ck, cv, cos, sin, fbuf, gbuf, qt, kx, vx, s_tiles, m_tiles, acc, top, tot,
    in_sem, f_send, f_recv, g_send, g_recv, gz_send, gz_recv,
):
    loads = [
        pltpu.make_async_copy(src, dst, in_sem.at[i])
        for i, (src, dst) in enumerate(((ck_hbm, ck), (cv_hbm, cv), (sk_hbm, sk), (sv_hbm, sv), (q_hbm, q)))
    ]
    for c in loads:
        c.start()
    me = lax.axis_index("ctx")
    column, z = me // nz, me % nz
    other = (1 - column) * nz + z

    def mine(d):
        return column * nz + (z + d + nz) % nz

    def theirs(d):
        return (1 - column) * nz + (z + d + nz) % nz

    up, down = mine(1), mine(-1)

    barrier = pltpu.get_barrier_semaphore()
    for peer in (up, down, other):
        pl.semaphore_signal(barrier, inc=1, device_id={"ctx": peer}, device_id_type=MESH)

    rows, count, heads, size = q.shape
    half = size // 2
    group = TILE // heads
    tiles = count // group
    piece = fbuf.shape[2]
    blk = piece // 2
    swap = flag[0] == 1
    scale = math.log2(math.e) / math.sqrt(size)
    cached = jnp.where(swap, clen[1], clen[0])
    live = (jnp.where(swap, nlen[1], nlen[0]), jnp.where(swap, nlen[0], nlen[1]))
    lane = lax.broadcasted_iota(jnp.int32, (piece, size), 1)
    line = lax.broadcasted_iota(jnp.int32, (piece, size), 0)

    def logical(slot, i):
        first, second = order[2 * slot], order[2 * slot + 1]
        return jnp.where(i < blk, first * blk + i, second * blk + i - blk)

    def pick(ref, r, at=slice(None)):
        return jnp.where(swap, ref[1 - r, at].astype(jnp.float32), ref[r, at].astype(jnp.float32))

    loads[0].wait()
    loads[1].wait()
    for h in range(2):
        at = slice(h * piece, (h + 1) * piece)
        gbuf[me, h] = pick(ck, 0, at).astype(jnp.bfloat16)
        gbuf[me, 2 + h] = pick(cv, 0, at).T.astype(jnp.bfloat16)
    loads[2].wait()
    loads[3].wait()
    k = (lane % half).astype(jnp.float32)
    inverse = jnp.exp2(k * (-2.0 / size * math.log2(ROPE_BASE)))
    sign = jnp.where(lane < half, -1.0, 1.0)
    index = logical(me, line)
    for r, base in enumerate((cached, 0)):
        cos[r], sin[r] = turn_tables((index + base).astype(jnp.float32), inverse, sign)
        x = pick(sk, r)
        fbuf[me, r] = (x * cos[r] + pltpu.roll(x, half, 1) * sin[r]).astype(jnp.bfloat16)
        fbuf[me, 2 + r] = pick(sv, r).T.astype(jnp.bfloat16)

    pl.semaphore_wait(barrier, 3)
    started = []
    counts = {"f": 0, "g": 0, "z": 0}
    sends = {"f": f_send, "g": g_send, "z": gz_send}
    recvs = {"f": f_recv, "g": g_recv, "z": gz_recv}

    def send(kind, src, dst, slot, peer):
        c = pltpu.make_async_remote_copy(
            src_ref=src, dst_ref=dst, send_sem=sends[kind].at[counts[kind]], recv_sem=recvs[kind].at[slot],
            device_id={"ctx": peer}, device_id_type=MESH,
        )
        counts[kind] += 1
        c.start()
        started.append(c)

    def send_f(slot, peer):
        send("f", fbuf.at[slot], fbuf.at[slot], slot, peer)

    def send_g(slot, peer):
        send("g", gbuf.at[slot], gbuf.at[slot], slot, peer)

    def send_half(slot, part, peer):
        ref = gbuf.at[slot, pl.ds(2 * part, 2)]
        send("z", ref, ref, part, peer)

    def got(buf, sem):
        pltpu.make_async_remote_copy(
            src_ref=buf, dst_ref=buf, send_sem=f_send.at[0], recv_sem=sem, device_id={"ctx": other}, device_id_type=MESH
        ).wait_recv()

    def got_f(slot):
        got(fbuf.at[slot], f_recv.at[slot])

    def got_g(slot):
        got(gbuf.at[slot], g_recv.at[slot])

    send_g(me, up)
    send_g(me, down)
    send_f(me, other)
    send_f(me, up)
    send_f(me, down)
    send_g(me, other)

    loads[4].wait()
    vx[:, size:] = jnp.ones((2, 16, vx.shape[2]), jnp.bfloat16)

    def prepare(t, _):
        here = pl.ds(pl.multiple_of(t * group, group), group)
        place = t * group + lax.broadcasted_iota(jnp.int32, (size, TILE), 1) // heads
        hot = jnp.where(lax.broadcasted_iota(jnp.int32, (size, TILE), 0) == place, 1.0, 0.0).astype(jnp.bfloat16)
        for r in range(rows):
            at = r * tiles + t
            x = pick(q, r, here)
            y = x * cos[r, here][:, None, :] + pltpu.roll(x, half, 2) * sin[r, here][:, None, :]
            qt[at, 0:size] = y.reshape(TILE, size).T.astype(jnp.bfloat16)
            qt[at, size : 2 * size] = hot
            acc[at] = jnp.zeros((size, TILE), jnp.float32)
            top[at] = jnp.full((1, TILE), NEG, jnp.float32)
            tot[at] = jnp.zeros((1, TILE), jnp.float32)
        return 0

    lax.fori_loop(0, tiles, prepare, 0)

    q_index = logical(me, lane)

    def bias(visible):
        return jnp.where(visible, 0.0, NEG).astype(jnp.bfloat16)

    def scores(t, at, row, keys):
        s = jnp.dot(kx[row, 0:keys], qt[at], preferred_element_type=jnp.float32)
        s_tiles[t][0:keys] = s
        m_tiles[t][...] = jnp.max(s, axis=0, keepdims=True)

    def absorb(t, at, row, keys):
        old = top[at]
        new = jnp.maximum(old, m_tiles[t][...])
        p = jnp.exp2((s_tiles[t][0:keys] - new) * scale)
        fade = jnp.exp2((old - new) * scale)
        both = jnp.dot(vx[row, :, 0:keys], p.astype(jnp.bfloat16), preferred_element_type=jnp.float32)
        acc[at] = acc[at] * fade + both[0:size]
        tot[at] = tot[at] * fade + both[size : size + 1]
        top[at] = new

    def compute(row, keys):
        ahead = 4
        for t in range(ahead):
            scores(t, row * tiles + t, row, keys)
        for t in range(tiles):
            if t + ahead < tiles:
                scores(t + ahead, row * tiles + t + ahead, row, keys)
            absorb(t, row * tiles + t, row, keys)

    def cache_chunk(*blocks):
        for j, (ref, slot) in enumerate(blocks):
            for h in range(2):
                at = (2 * j + h) * piece
                kx[0, at : at + piece, 0:size] = ref[h]
                kx[0, at : at + piece, size : 2 * size] = bias(slot * 2 * piece + h * piece + line < cached)
                vx[0, 0:size, at : at + piece] = ref[2 + h]
        compute(0, 2 * piece * len(blocks))

    def span_chunk(*blocks):
        for j, (ref, slot) in enumerate(blocks):
            at = j * piece
            k_index = logical(slot, line)
            for r in range(2):
                kx[r, at : at + piece, 0:size] = ref[r]
                kx[r, at : at + piece, size : 2 * size] = bias((k_index <= q_index) & (k_index < live[r]))
                vx[r, 0:size, at : at + piece] = ref[2 + r]

        def one(r, _):
            compute(r, piece * len(blocks))
            return 0

        lax.fori_loop(0, 2, one, 0)

    def gb(slot):
        return gbuf.at[slot], slot

    def fb(slot):
        return fbuf.at[slot], slot

    last = nz // 2

    def on(d):
        return down if d > 0 else up

    def pass_f(*slots):
        for slot, d in slots:
            got_f(slot)
            send_f(slot, on(d))

    def pass_g(*distances):
        for d in distances:
            got_g(mine(d))
            send_g(mine(d), on(d))
            send_g(mine(d), other)

    got_f(other)
    send_f(other, up)
    send_f(other, down)
    pass_g(1, -1)
    cache_chunk(gb(mine(1)), gb(mine(-1)))
    pass_f((mine(1), 1), (mine(-1), -1))
    got_g(other)
    cache_chunk(gb(me), gb(other))
    span_chunk(fb(me), fb(other), fb(mine(1)), fb(mine(-1)))
    pass_f((theirs(1), 1), (theirs(-1), -1))
    pass_g(2, -2)
    got_g(theirs(1))
    got_g(theirs(-1))
    cache_chunk(gb(theirs(1)), gb(theirs(-1)))
    cache_chunk(gb(mine(2)), gb(mine(-2)))
    pass_f((mine(2), 2), (mine(-2), -2))
    span_chunk(fb(theirs(1)), fb(theirs(-1)), fb(mine(2)), fb(mine(-2)))
    pass_f((theirs(2), 2), (theirs(-2), -2))
    for d in (3, -3):
        got_g(mine(d))
        send_half(mine(d), 0 if d < 0 else 1, on(d))
        send_g(mine(d), other)
    got_g(theirs(2))
    got_g(theirs(-2))
    cache_chunk(gb(theirs(2)), gb(theirs(-2)))
    cache_chunk(gb(mine(3)), gb(mine(-3)))
    got_f(mine(3))
    got_f(mine(-3))
    send_f(mine(-3), up)
    span_chunk(fb(theirs(2)), fb(theirs(-2)), fb(mine(3)), fb(mine(-3)))
    got_f(theirs(3))
    got_f(theirs(-3))
    send_f(theirs(3), down)
    span_chunk(fb(theirs(3)), fb(theirs(-3)))
    far = mine(nz // 2)
    for part in range(2):
        got(gbuf.at[far, pl.ds(2 * part, 2)], gz_recv.at[part])
    send_g(far, other)
    got_g(theirs(3))
    got_g(theirs(-3))
    cache_chunk(gb(theirs(3)), gb(theirs(-3)))
    cache_chunk(gb(far))
    got_f(far)
    got_f(theirs(nz // 2))
    span_chunk(fb(far), fb(theirs(nz // 2)))
    got_g(theirs(nz // 2))
    cache_chunk(gb(theirs(nz // 2)))

    def finish(t, _):
        here = pl.ds(pl.multiple_of(t * group, group), group)
        done = [(acc[r * tiles + t] / tot[r * tiles + t]).T.reshape(group, heads, size) for r in range(2)]
        i = logical(me, t * group + lax.broadcasted_iota(jnp.int32, (group, heads, size), 0))
        for r in range(2):
            value = jnp.where(swap, done[1 - r], done[r])
            out[r, here] = jnp.where(i < nlen[r], value, 0.0).astype(out.dtype)
        return 0

    lax.fori_loop(0, tiles, finish, 0)
    for c in started:
        c.wait_send()


def shards(nz, queries, span_k, span_v, cache_k, cache_v, cached_len, new_len, prefill_flag, block_order):
    rows, count, heads, size = queries.shape
    n_ctx = lax.axis_size("ctx")
    smem = pl.BlockSpec(memory_space=pltpu.SMEM)
    hbm = pl.BlockSpec(memory_space=pl.ANY)
    vmem = pl.BlockSpec(memory_space=pltpu.VMEM)
    tiles = count * heads // TILE
    keys = 4 * count
    bf16, f32, dma = jnp.bfloat16, jnp.float32, pltpu.SemaphoreType.DMA
    inputs = [queries] + [a[:, :, 0] for a in (span_k, span_v, cache_k, cache_v)]
    placed = [pltpu.with_memory_space_constraint(a, pltpu.HBM) for a in inputs]
    scalars = [pltpu.with_memory_space_constraint(a, pltpu.HBM) for a in (prefill_flag, cached_len, new_len, block_order)]
    return pl.pallas_call(
        functools.partial(main_kernel, nz),
        out_shape=jax.ShapeDtypeStruct(queries.shape, queries.dtype),
        in_specs=[smem] * 4 + [hbm] * 5,
        out_specs=vmem,
        scratch_shapes=[pltpu.VMEM(a.shape, bf16) for a in inputs]
        + [
            pltpu.VMEM((rows, count, size), f32),
            pltpu.VMEM((rows, count, size), f32),
            pltpu.VMEM((n_ctx, 4, count, size), bf16),
            pltpu.VMEM((n_ctx, 4, count, size), bf16),
            pltpu.VMEM((2 * tiles, 2 * size, TILE), bf16),
            pltpu.VMEM((2, keys, 2 * size), bf16),
            pltpu.VMEM((2, size + 16, keys), bf16),
            [pltpu.VMEM((keys, TILE), f32)] * tiles,
            [pltpu.VMEM((1, TILE), f32)] * tiles,
            pltpu.VMEM((2 * tiles, size, TILE), f32),
            pltpu.VMEM((2 * tiles, 1, TILE), f32),
            pltpu.VMEM((2 * tiles, 1, TILE), f32),
            dma((5,)),
            dma((2 * n_ctx,)),
            dma((n_ctx,)),
            dma((2 * n_ctx,)),
            dma((n_ctx,)),
            dma((2,)),
            dma((2,)),
        ],
        compiler_params=pltpu.CompilerParams(collective_id=0, has_side_effects=True, vmem_limit_bytes=51 * 1024 * 1024),
        name="gather_attend",
    )(*scalars, *placed)


def solution(mesh):
    nz = mesh.shape["ctx"] // 2
    four = P("batch", "ctx", "tp", None)
    return jax.shard_map(
        functools.partial(shards, nz),
        mesh=mesh,
        in_specs=(four,) * 5 + (P("batch"),) * 3 + (P(),),
        out_specs=four,
        check_vma=False,
    )
```

```python
import functools
import math

import jax
import jax.numpy as jnp
from jax import lax
from jax.experimental import pallas as pl
from jax.experimental.pallas import tpu as pltpu
from jax.sharding import PartitionSpec as P

ROPE_BASE = 500000.0
NEG = -1e30
TILE = 256
MESH = pl.DeviceIdType.MESH


HALF_PI = (1.5703125, 4.837512969970703125e-4, 7.54978995489188216e-8)


def turn_tables(positions, inverse, sign):
    angle = positions * inverse
    quarter = jnp.floor(angle * (2.0 / math.pi) + 0.5)
    x = ((angle - quarter * HALF_PI[0]) - quarter * HALF_PI[1]) - quarter * HALF_PI[2]
    z = x * x
    sine = ((-1.9515295891e-4 * z + 8.3321608736e-3) * z - 1.6666654611e-1) * z * x + x
    cosine = ((2.443315711809948e-5 * z - 1.388731625493765e-3) * z + 4.166664568298827e-2) * z * z - 0.5 * z + 1.0
    n = quarter.astype(jnp.int32)
    odd = (n & 1) == 1
    c = jnp.where(odd, sine, cosine)
    s = jnp.where(odd, cosine, sine)
    c = jnp.where(((n + 1) & 2) == 2, -c, c)
    s = jnp.where((n & 2) == 2, -s, s)
    return c, s * sign


def main_kernel(
    nz, flag, clen, nlen, order, q_hbm, sk_hbm, sv_hbm, ck_hbm, cv_hbm, out,
    q, sk, sv, ck, cv, cos, sin, fbuf, gbuf, qt, kx, vx, s_tiles, m_tiles, acc, top, tot,
    in_sem, f_send, f_recv, g_send, g_recv, h_send, h_recv,
):
    loads = [
        pltpu.make_async_copy(src, dst, in_sem.at[i])
        for i, (src, dst) in enumerate(((ck_hbm, ck), (cv_hbm, cv), (sk_hbm, sk), (sv_hbm, sv), (q_hbm, q)))
    ]
    for c in loads:
        c.start()
    me = lax.axis_index("ctx")
    column, z = me // nz, me % nz
    other = (1 - column) * nz + z

    def mine(d):
        return column * nz + (z + d + nz) % nz

    def theirs(d):
        return (1 - column) * nz + (z + d + nz) % nz

    up, down = mine(1), mine(-1)

    barrier = pltpu.get_barrier_semaphore()
    for peer in (up, down, other):
        pl.semaphore_signal(barrier, inc=1, device_id={"ctx": peer}, device_id_type=MESH)

    rows, count, heads, size = q.shape
    half = size // 2
    group = TILE // heads
    tiles = count // group
    piece = fbuf.shape[2]
    blk = piece // 2
    swap = flag[0] == 1
    scale = math.log2(math.e) / math.sqrt(size)
    cached = jnp.where(swap, clen[1], clen[0])
    live = (jnp.where(swap, nlen[1], nlen[0]), jnp.where(swap, nlen[0], nlen[1]))
    lane = lax.broadcasted_iota(jnp.int32, (piece, size), 1)
    line = lax.broadcasted_iota(jnp.int32, (piece, size), 0)

    def logical(slot, i):
        first, second = order[2 * slot], order[2 * slot + 1]
        return jnp.where(i < blk, first * blk + i, second * blk + i - blk)

    def pick(ref, r, at=slice(None)):
        return jnp.where(swap, ref[1 - r, at].astype(jnp.float32), ref[r, at].astype(jnp.float32))

    loads[0].wait()
    loads[1].wait()
    for h in range(2):
        at = slice(h * piece, (h + 1) * piece)
        gbuf[me, h] = pick(ck, 0, at).astype(jnp.bfloat16)
        gbuf[me, 2 + h] = pick(cv, 0, at).T.astype(jnp.bfloat16)
    loads[2].wait()
    loads[3].wait()
    k = (lane % half).astype(jnp.float32)
    inverse = jnp.exp2(k * (-2.0 / size * math.log2(ROPE_BASE)))
    sign = jnp.where(lane < half, -1.0, 1.0)
    index = logical(me, line)
    for r, base in enumerate((cached, 0)):
        cos[r], sin[r] = turn_tables((index + base).astype(jnp.float32), inverse, sign)
        x = pick(sk, r)
        fbuf[me, r] = (x * cos[r] + pltpu.roll(x, half, 1) * sin[r]).astype(jnp.bfloat16)
        fbuf[me, 2 + r] = pick(sv, r).T.astype(jnp.bfloat16)

    pl.semaphore_wait(barrier, 3)
    started = []
    counts = {"f": 0, "g": 0, "h": 0}
    sends = {"f": f_send, "g": g_send, "h": h_send}
    recvs = {"f": f_recv, "g": g_recv, "h": h_recv}

    def send(kind, src, dst, slot, peer):
        c = pltpu.make_async_remote_copy(
            src_ref=src, dst_ref=dst, send_sem=sends[kind].at[counts[kind]], recv_sem=recvs[kind].at[slot],
            device_id={"ctx": peer}, device_id_type=MESH,
        )
        counts[kind] += 1
        c.start()
        started.append(c)

    def send_f(slot, peer):
        send("f", fbuf.at[slot], fbuf.at[slot], slot, peer)

    def send_g(slot, peer):
        send("g", gbuf.at[slot], gbuf.at[slot], slot, peer)

    def half_of(slot, part):
        return fbuf.at[slot, pl.ds(2 * part, 2)]

    def send_half(slot, part, peer):
        send("h", half_of(slot, part), half_of(slot, part), part, peer)

    def got(buf, sem):
        pltpu.make_async_remote_copy(
            src_ref=buf, dst_ref=buf, send_sem=f_send.at[0], recv_sem=sem, device_id={"ctx": other}, device_id_type=MESH
        ).wait_recv()

    def got_f(slot):
        got(fbuf.at[slot], f_recv.at[slot])

    def got_half(slot, part):
        got(half_of(slot, part), h_recv.at[part])

    def got_g(slot):
        got(gbuf.at[slot], g_recv.at[slot])

    send_g(me, up)
    send_g(me, down)
    send_f(me, other)
    send_f(me, up)
    send_f(me, down)
    send_g(me, other)

    vx[:, size:] = jnp.ones((3, 16, vx.shape[2]), jnp.bfloat16)

    loads[4].wait()

    def prepare(t, _):
        here = pl.ds(pl.multiple_of(t * group, group), group)
        place = t * group + lax.broadcasted_iota(jnp.int32, (size, TILE), 1) // heads
        hot = jnp.where(lax.broadcasted_iota(jnp.int32, (size, TILE), 0) == place, 1.0, 0.0).astype(jnp.bfloat16)
        for r in range(rows):
            at = r * tiles + t
            x = pick(q, r, here)
            y = x * cos[r, here][:, None, :] + pltpu.roll(x, half, 2) * sin[r, here][:, None, :]
            qt[at, 0:size] = y.reshape(TILE, size).T.astype(jnp.bfloat16)
            qt[at, size : 2 * size] = hot
            acc[at] = jnp.zeros((size, TILE), jnp.float32)
            top[at] = jnp.full((1, TILE), NEG, jnp.float32)
            tot[at] = jnp.zeros((1, TILE), jnp.float32)
        return 0

    lax.fori_loop(0, tiles, prepare, 0)

    q_index = logical(me, lane)

    def bias(visible):
        return jnp.where(visible, 0.0, NEG).astype(jnp.bfloat16)

    def scores(t, at, buf, keys):
        s = jnp.dot(kx[buf, 0:keys], qt[at], preferred_element_type=jnp.float32)
        s_tiles[t][0:keys] = s
        m_tiles[t][...] = jnp.max(s, axis=0, keepdims=True)

    def absorb(t, at, buf, keys):
        old = top[at]
        new = jnp.maximum(old, m_tiles[t][...])
        p = jnp.exp2((s_tiles[t][0:keys] - new) * scale)
        fade = jnp.exp2((old - new) * scale)
        both = jnp.dot(vx[buf, :, 0:keys], p.astype(jnp.bfloat16), preferred_element_type=jnp.float32)
        acc[at] = acc[at] * fade + both[0:size]
        tot[at] = tot[at] * fade + both[size : size + 1]
        top[at] = new

    def compute(row, keys, buf):
        ahead = 4 if keys > TILE else tiles
        for t in range(ahead):
            scores(t, row * tiles + t, buf, keys)
        for t in range(tiles):
            if t + ahead < tiles:
                scores(t + ahead, row * tiles + t + ahead, buf, keys)
            absorb(t, row * tiles + t, buf, keys)

    def cache_operands(*blocks):
        for j, (ref, slot) in enumerate(blocks):
            for h in range(2):
                at = (2 * j + h) * piece
                kx[2, at : at + piece, 0:size] = ref[h]
                kx[2, at : at + piece, size : 2 * size] = bias(slot * 2 * piece + h * piece + line < cached)
                vx[2, 0:size, at : at + piece] = ref[2 + h]

    def cache_chunk(*blocks):
        cache_operands(*blocks)
        compute(0, 2 * piece * len(blocks), 2)

    def span_operands(*blocks):
        for j, (ref, slot) in enumerate(blocks):
            at = j * piece
            k_index = logical(slot, line)
            for r in range(2):
                kx[r, at : at + piece, 0:size] = ref[r]
                kx[r, at : at + piece, size : 2 * size] = bias((k_index <= q_index) & (k_index < live[r]))
                vx[r, 0:size, at : at + piece] = ref[2 + r]

    def span_chunk(*blocks):
        span_operands(*blocks)

        def one(r, _):
            compute(r, piece * len(blocks), r)
            return 0

        lax.fori_loop(0, 2, one, 0)

    def gb(slot):
        return gbuf.at[slot], slot

    def fb(slot):
        return fbuf.at[slot], slot

    last = nz // 2

    def on(d):
        return down if d > 0 else up

    got_f(other)
    send_f(other, down)
    send_f(other, up)
    for d in (1, -1):
        got_g(mine(d))
        send_g(mine(d), on(d))
        send_g(mine(d), other)
    cache_chunk(gb(mine(1)), gb(mine(-1)))
    for d in (1, -1):
        got_f(mine(d))
        send_f(mine(d), on(d))
    got_g(other)
    cache_chunk(gb(me), gb(other))
    span_chunk(fb(me), fb(other), fb(mine(1)), fb(mine(-1)))
    for d in (1, -1):
        got_f(theirs(d))
        send_f(theirs(d), on(d))
    for d in (2, -2):
        got_g(mine(d))
        send_g(mine(d), on(d))
        send_g(mine(d), other)
    cache_chunk(gb(mine(2)), gb(mine(-2)))
    for d in (2, -2):
        got_f(mine(d))
        send_f(mine(d), on(d))
    span_chunk(fb(theirs(1)), fb(theirs(-1)), fb(mine(2)), fb(mine(-2)))
    got_g(theirs(1))
    got_g(theirs(-1))
    cache_chunk(gb(theirs(1)), gb(theirs(-1)))
    got_f(theirs(2))
    send_f(theirs(2), down)
    got_g(mine(-3))
    send_g(mine(-3), up)
    got_g(mine(3))
    send_g(mine(3), other)
    send_g(mine(-3), other)
    got_f(theirs(-2))
    send_f(theirs(-2), up)
    cache_chunk(gb(mine(3)), gb(mine(-3)))
    got_g(theirs(2))
    got_g(theirs(-2))
    cache_chunk(gb(theirs(2)), gb(theirs(-2)))
    got_f(mine(3))
    send_half(mine(3), 1, down)
    got_f(mine(-3))
    send_half(mine(-3), 0, up)
    span_chunk(fb(theirs(2)), fb(theirs(-2)), fb(mine(3)), fb(mine(-3)))
    far, far_other = mine(nz // 2), theirs(nz // 2)
    got_f(theirs(3))
    send_f(theirs(3), down)
    got_g(far)
    send_g(far, other)
    got_g(theirs(3))
    cache_chunk(gb(far), gb(theirs(3)))
    got_g(theirs(-3))
    cache_chunk(gb(theirs(-3)))
    got_f(theirs(-3))
    span_chunk(fb(theirs(3)), fb(theirs(-3)))
    got_half(far, 0)
    got_half(far, 1)
    got_f(far_other)
    got_g(far_other)
    cache_operands(gb(far_other))
    span_operands(fb(far), fb(far_other))
    compute(0, 2 * piece, 2)
    compute(1, 2 * piece, 1)
    compute(0, 2 * piece, 0)

    def finish(t, _):
        here = pl.ds(pl.multiple_of(t * group, group), group)
        done = [(acc[r * tiles + t] / tot[r * tiles + t]).T.reshape(group, heads, size) for r in range(2)]
        i = logical(me, t * group + lax.broadcasted_iota(jnp.int32, (group, heads, size), 0))
        for r in range(2):
            value = jnp.where(swap, done[1 - r], done[r])
            out[r, here] = jnp.where(i < nlen[r], value, 0.0).astype(out.dtype)
        return 0

    lax.fori_loop(0, tiles, finish, 0)
    for c in started:
        c.wait_send()


def shards(nz, queries, span_k, span_v, cache_k, cache_v, cached_len, new_len, prefill_flag, block_order):
    rows, count, heads, size = queries.shape
    n_ctx = lax.axis_size("ctx")
    smem = pl.BlockSpec(memory_space=pltpu.SMEM)
    hbm = pl.BlockSpec(memory_space=pl.ANY)
    vmem = pl.BlockSpec(memory_space=pltpu.VMEM)
    tiles = count * heads // TILE
    keys = 4 * count
    bf16, f32, dma = jnp.bfloat16, jnp.float32, pltpu.SemaphoreType.DMA
    inputs = [queries] + [a[:, :, 0] for a in (span_k, span_v, cache_k, cache_v)]
    placed = [pltpu.with_memory_space_constraint(a, pltpu.HBM) for a in inputs]
    scalars = [pltpu.with_memory_space_constraint(a, pltpu.HBM) for a in (prefill_flag, cached_len, new_len, block_order)]
    return pl.pallas_call(
        functools.partial(main_kernel, nz),
        out_shape=jax.ShapeDtypeStruct(queries.shape, queries.dtype),
        in_specs=[smem] * 4 + [hbm] * 5,
        out_specs=vmem,
        scratch_shapes=[pltpu.VMEM(a.shape, bf16) for a in inputs]
        + [
            pltpu.VMEM((rows, count, size), f32),
            pltpu.VMEM((rows, count, size), f32),
            pltpu.VMEM((n_ctx, 4, count, size), bf16),
            pltpu.VMEM((n_ctx, 4, count, size), bf16),
            pltpu.VMEM((2 * tiles, 2 * size, TILE), bf16),
            pltpu.VMEM((3, keys, 2 * size), bf16),
            pltpu.VMEM((3, size + 16, keys), bf16),
            [pltpu.VMEM((keys, TILE), f32)] * tiles,
            [pltpu.VMEM((1, TILE), f32)] * tiles,
            pltpu.VMEM((2 * tiles, size, TILE), f32),
            pltpu.VMEM((2 * tiles, 1, TILE), f32),
            pltpu.VMEM((2 * tiles, 1, TILE), f32),
            dma((5,)),
            dma((2 * n_ctx,)),
            dma((n_ctx,)),
            dma((2 * n_ctx,)),
            dma((n_ctx,)),
            dma((2,)),
            dma((2,)),
        ],
        compiler_params=pltpu.CompilerParams(collective_id=0, has_side_effects=True, vmem_limit_bytes=51 * 1024 * 1024),
        name="gather_attend",
    )(*scalars, *placed)


def solution(mesh):
    nz = mesh.shape["ctx"] // 2
    four = P("batch", "ctx", "tp", None)
    return jax.shard_map(
        functools.partial(shards, nz),
        mesh=mesh,
        in_specs=(four,) * 5 + (P("batch"),) * 3 + (P(),),
        out_specs=four,
        check_vma=False,
    )
```
